32 devices in a mesh: rows: 16 (over z, y, x), cols: 2 (over core).
Axes of the slice: x: 2, y: 2, z: 4, core: 2. Of those that a mesh axis runs over, the one named last changes fastest.
Arguments:
- design: float32 [16384, 512], P('rows', 'cols'), may hold values from -24 to 24
- signs: int32 [16384], P('rows'), may hold values from -1 to 1, as said below
- kept: int32 [1024], replicated, may hold values from 0 to 16383, as said below
Outputs:
- sketch: float32 [1024, 512], P('rows', 'cols')
- factor: float32 [512, 512], P(None, 'cols')
The draws below stay inside these ranges and needn't reach their ends.
Inputs may be any that keep to these rules, and one draw needn't show every extreme that they name: `signs`: each entry is +1 or -1. `kept`: distinct and increasing.
All inputs are finite; a program needn't handle non-finite values.
Results may differ from the reference program's by a relative error of at most 0.0003.
Values sent between devices are 32-bit elements; how exact they have to be, the bound alone decides.
A program may use at most 64 MiB of HBM per device.

```python
import math
import jax
import jax.numpy as jnp
from jax import lax

P_SIZE = 512
ROWS_DEV = 1024
ROWS = 16384
KEPT = 1024
N_ROWS = 16


def draw_design(key, part):
    base = jax.random.fold_in(key, 11)
    first, second, third = jax.random.split(base, 3)
    column_scales = jnp.exp(jax.random.uniform(first, (P_SIZE,), jnp.float32, jnp.log(0.3), jnp.log(3.0)))
    noise = jax.random.normal(second, (ROWS, P_SIZE), jnp.float32)
    common = jax.random.normal(third, (ROWS, 1), jnp.float32)
    values = (noise + 0.6 * common) * column_scales[None, :]
    return jnp.clip(values, -24.0, 24.0).astype(jnp.float32)


def draw_signs(key, part):
    base = jax.random.fold_in(key, 22)
    return (2 * jax.random.randint(base, (ROWS,), 0, 2) - 1).astype(jnp.int32)


def draw_kept(key, part):
    base = jax.random.fold_in(key, 33)
    chosen = jax.random.permutation(base, ROWS)[:KEPT]
    return jnp.sort(chosen).astype(jnp.int32)


def setup_inputs(seed: int = 0) -> dict:
    arg_keys = jax.random.split(jax.random.key(seed), 4)
    design = draw_design(jax.random.fold_in(arg_keys[3], 71), 0)
    signs = draw_signs(jax.random.fold_in(arg_keys[3], 71), 0)
    kept = draw_kept(jax.random.fold_in(arg_keys[3], 71), 0)
    return dict(design=design, signs=signs, kept=kept)


def hadamard(order):
    matrix = jnp.ones((1, 1), jnp.float32)
    base = jnp.array([[1.0, 1.0], [1.0, -1.0]], jnp.float32)
    while matrix.shape[0] < order:
        matrix = jnp.kron(matrix, base)
    return matrix

def bit_parity(value):
    folded = value.astype(jnp.int32)
    for amount in (16, 8, 4, 2, 1):
        folded = jnp.bitwise_xor(folded, jnp.right_shift(folded, amount))
    return jnp.bitwise_and(folded, 1)

def local_transform(flipped):
    length, width = flipped.shape
    outer = length // 128
    inner_table = hadamard(128)
    outer_table = hadamard(outer)
    blocks = flipped.reshape(outer, 128, width)
    mixed = jnp.einsum('pb,abc->apc', inner_table, blocks, precision=lax.Precision.HIGHEST)
    mixed = jnp.einsum('qa,apc->qpc', outer_table, mixed, precision=lax.Precision.HIGHEST)
    return mixed.reshape(length, width)

def reference(design, signs, kept):
    length = ROWS_DEV
    kept_blocks = (kept // length).astype(jnp.int32)
    offsets = (kept - kept_blocks * length).astype(jnp.int32)
    scale = 1.0 / math.sqrt(ROWS)

    def step(total, block_row):
        start = (block_row * length).astype(jnp.int32)
        piece = lax.dynamic_slice_in_dim(design, start, length, 0)
        flips = lax.dynamic_slice_in_dim(signs, start, length, 0)
        transformed = local_transform(piece * flips.astype(jnp.float32)[:, None])
        parity = bit_parity(jnp.bitwise_and(kept_blocks, block_row))
        factor = (1.0 - 2.0 * parity.astype(jnp.float32)) * scale
        return (total + jnp.take(transformed, offsets, axis=0) * factor[:, None], None)
    start_total = jnp.zeros((KEPT, P_SIZE), jnp.float32)
    sketch, unused = lax.scan(step, start_total, jnp.arange(N_ROWS, dtype=jnp.int32))
    gram = jnp.dot(sketch.T.astype(jnp.float32), sketch.astype(jnp.float32), precision=lax.Precision.HIGHEST, preferred_element_type=jnp.float32) / KEPT
    factor = jnp.linalg.cholesky(gram).T
    return (sketch, factor)
```

```python
import functools
import math

import jax
import jax.numpy as jnp
from jax import lax
from jax.experimental import pallas as pl
from jax.experimental.pallas import tpu as pltpu
from jax.sharding import PartitionSpec as P

MESH = pl.DeviceIdType.MESH
HIGHEST = lax.Precision.HIGHEST
LANES = 128


def transform_kernel(scale, tile, design_ref, signs_ref, kept_ref, out_ref, split):
    length = design_ref.shape[0]
    values = design_ref[...]
    high = values.astype(jnp.bfloat16)
    split[0] = high
    split[1] = (values - high.astype(jnp.float32)).astype(jnp.bfloat16)
    first_row = lax.axis_index("rows") * length
    lane = lax.broadcasted_iota(jnp.int32, (LANES, LANES), 1)

    def step(index, carry):
        stacked = []
        for piece in range(tile // LANES):
            row = kept_ref[pl.ds(index * (tile // LANES) + piece, 1), :]
            column = jnp.broadcast_to(row, (LANES, LANES)).T
            blocks = []
            for block in range(length // LANES):
                common = jnp.bitwise_and(column, lane + (first_row + block * LANES))
                odd = jnp.bitwise_and(lax.population_count(common), 1)
                flips = signs_ref[block : block + 1, :]
                entry = (1 - 2 * odd) * flips
                blocks.append(entry.astype(jnp.float32).astype(jnp.bfloat16))
            stacked.append(jnp.concatenate(blocks, axis=1))
        table = jnp.concatenate(stacked, axis=0)
        total = jnp.dot(table, split[1], preferred_element_type=jnp.float32)
        total += jnp.dot(table, split[0], preferred_element_type=jnp.float32)
        out_ref[pl.ds(pl.multiple_of(index * tile, tile), tile), :] = total * scale
        return carry

    lax.fori_loop(0, out_ref.shape[0] // tile, step, 0)


def transform(design, signs, kept, total_rows):
    length, width = design.shape
    count = kept.shape[0]
    tile = 256
    return pl.pallas_call(
        functools.partial(transform_kernel, 1.0 / math.sqrt(total_rows), tile),
        out_shape=jax.ShapeDtypeStruct((count, width), jnp.float32),
        in_specs=[pl.BlockSpec(memory_space=pltpu.VMEM)] * 3,
        out_specs=pl.BlockSpec(memory_space=pltpu.VMEM),
        scratch_shapes=[pltpu.VMEM((2, length, width), jnp.bfloat16)],
        cost_estimate=pl.CostEstimate(
            flops=4 * count * length * width, bytes_accessed=4 * (count + length) * width, transcendentals=0
        ),
    )(design, signs.reshape(-1, LANES), kept.reshape(-1, LANES))


def exchange_kernel(
    n, orders, x_ref, sketch_ref, gram_ref, buf, recv, gat,
    rs_send, rs_recv, ag_send, ag_recv, ex_send, ex_recv,
):
    me = lax.axis_index("rows")
    core = lax.axis_index("cols")
    levels = len(orders[0])
    parts = len(orders)
    width = x_ref.shape[2]
    sub = x_ref.shape[1] // parts

    def flip(bit):
        return (1 - 2 * ((me // (1 << bit)) % 2)) * (1 << bit)

    barrier = pltpu.get_barrier_semaphore()
    for bit in range(levels):
        pl.semaphore_signal(barrier, inc=1, device_id=(me + flip(bit), core), device_id_type=MESH)
    far = flip(levels - 1) + flip(levels - 2)
    pl.semaphore_signal(barrier, inc=1, device_id=(me + far, core), device_id_type=MESH)
    pl.semaphore_signal(barrier, inc=1, device_id=(me, 1 - core), device_id_type=MESH)

    def slot_owner(part, slot):
        owner = me
        for place, bit in enumerate(orders[part]):
            if (slot >> (levels - 1 - place)) & 1:
                owner = owner + flip(bit)
        return owner

    lanes = pl.ds(pl.multiple_of(core * width, LANES), width)

    for part in range(parts):
        for slot in range(n - 1, -1, -1):
            buf[part, slot] = x_ref[slot_owner(part, slot), part * sub : (part + 1) * sub, :]
    pl.semaphore_wait(barrier, levels + 2)

    def level_of(slot):
        return levels - slot.bit_length()

    def partner(part, slot):
        return me + (far if slot == 3 else flip(orders[part][level_of(slot)]))

    def reduce_copy(part, slot):
        return pltpu.make_async_remote_copy(
            src_ref=buf.at[part, slot],
            dst_ref=recv.at[part, slot],
            send_sem=rs_send.at[part, slot],
            recv_sem=rs_recv.at[part, slot],
            device_id=(partner(part, slot), core),
            device_id_type=MESH,
        )

    for slot in range(n - 1, n // 2 - 1, -1):
        for part in range(parts):
            reduce_copy(part, slot).start()
    for slot in range(n // 2 - 1, -1, -1):
        for part in range(parts):
            total = buf[part, slot]
            terms = [slot + (1 << k) for k in range(levels - 1, -1, -1) if (1 << k) > slot]
            if slot == 1:
                terms.remove(3)
            if slot == 0:
                terms.append(3)
            for term in terms:
                reduce_copy(part, term).wait_recv()
                total += recv[part, term]
            if slot:
                buf[part, slot] = total
                reduce_copy(part, slot).start()
            else:
                sketch_ref[part * sub : (part + 1) * sub, :] = total
                gat[part, 0, :, lanes] = total

    def gather_copy(part, slot):
        source = 0 if slot == 3 else slot - (n >> (level_of(slot) + 1))
        return pltpu.make_async_remote_copy(
            src_ref=gat.at[part, source, :, lanes],
            dst_ref=gat.at[part, slot, :, lanes],
            send_sem=ag_send.at[part, slot],
            recv_sem=ag_recv.at[part, slot],
            device_id=(partner(part, slot), core),
            device_id_type=MESH,
        )

    def core_copy(part, slot):
        return pltpu.make_async_remote_copy(
            src_ref=gat.at[part, slot, :, lanes],
            dst_ref=gat.at[part, slot, :, lanes],
            send_sem=ex_send.at[part, slot],
            recv_sem=ex_recv.at[part, slot],
            device_id=(me, 1 - core),
            device_id_type=MESH,
        )

    def forward(part, slot):
        half = 1
        while half < n:
            if half > slot and slot + half != 3:
                gather_copy(part, slot + half).start()
            half *= 2
        if slot == 0:
            gather_copy(part, 3).start()
        core_copy(part, slot).start()

    def receive(slot):
        for part in range(parts):
            gather_copy(part, slot).wait_recv()
            forward(part, slot)

    def add_gram(start, size, first=False):
        whole = gat.shape[3]
        half = whole // 2
        group = min(size, 8)
        for slot in range(start, start + size):
            for part in range(parts):
                core_copy(part, slot).wait_recv()
        if first:
            gram_ref[...] = jnp.zeros_like(gram_ref)

        def step(index, carry):
            part, piece = index // (size // group), index % (size // group)
            rows = gat[part, pl.ds(start + piece * group, group)].reshape(group * sub, whole)
            dims = (((0,), (0,)), ((), ()))
            high, low = split3(rows)
            left = jnp.concatenate([high, high, low], axis=0)
            right = jnp.concatenate([high, low, high], axis=0)
            gram_ref[0:half, :] += lax.dot_general(
                left[:, :half], right, dims, preferred_element_type=jnp.float32
            )
            gram_ref[half:, half:] += lax.dot_general(
                left[:, half:], right[:, half:], dims, preferred_element_type=jnp.float32
            )
            return carry

        lax.fori_loop(0, parts * (size // group), step, 0)

    for part in range(parts):
        forward(part, 0)
    inner = sorted(range(1, n // 2), key=lambda slot: (slot.bit_count(), -slot))
    for slot in inner:
        receive(slot)
    add_gram(0, n // 2, True)
    for slot in range(n // 2, n):
        receive(slot)
    add_gram(n // 2, n // 2)
    for part in range(parts):
        for slot in range(n):
            if slot:
                reduce_copy(part, slot).wait_send()
                gather_copy(part, slot).wait_send()
            core_copy(part, slot).wait_send()


def exchange(outgoing, n, cores):
    count, width = outgoing.shape
    per = count // n
    levels = n.bit_length() - 1
    parts = 2
    orders = []
    for part in range(parts):
        order = list(range(levels))
        if part % 2 and levels > 1:
            order[0], order[1] = order[1], order[0]
        orders.append(tuple(order))
    slots = (parts, n, per // parts, width)
    sems = pltpu.SemaphoreType.DMA((parts, n))
    whole = width * cores
    return pl.pallas_call(
        functools.partial(exchange_kernel, n, tuple(orders)),
        out_shape=(
            jax.ShapeDtypeStruct((per, width), jnp.float32),
            jax.ShapeDtypeStruct((whole, whole), jnp.float32),
        ),
        in_specs=[pl.BlockSpec(memory_space=pltpu.VMEM)],
        out_specs=(pl.BlockSpec(memory_space=pltpu.VMEM),) * 2,
        scratch_shapes=[
            pltpu.VMEM(slots, jnp.float32),
            pltpu.VMEM(slots, jnp.float32),
            pltpu.VMEM((parts, n, per // parts, whole), jnp.float32),
            sems, sems, sems, sems, sems, sems,
        ],
        compiler_params=pltpu.CompilerParams(
            collective_id=0, has_side_effects=True, vmem_limit_bytes=60 * 1024 * 1024
        ),
    )(outgoing.reshape(n, per, width))


def spread(x, lane):
    return jnp.broadcast_to(x[:, lane:lane+1], x.shape)

def factor_panel(rows, first):
    depth = len(rows)
    tiles = len(rows[0])
    sub = lax.broadcasted_iota(jnp.int32, (8, LANES), 0)
    rows = [list(r) for r in rows]
    ahead = [[spread(rows[r][0], first + j) for r in range(depth)] for j in range(8)]
    done = []
    for g in range(depth):
        here = ahead
        if g + 1 < depth:
            ahead = [[spread(rows[r][0], first + 8 * (g + 1) + j) for r in range(g + 1, depth)] for j in range(8)]
        top = rows[g]
        for j in range(8):
            column = here[j]
            root = lax.rsqrt(column[0][j:j+1])
            root = jnp.broadcast_to(root, (8, LANES))
            scaled = [c * root for c in column]
            for later in range(j + 1, 8):
                weight = here[later][0][j:j+1] * root
                here[later] = [c - s * weight for c, s in zip(here[later], scaled)]
            below = jnp.where(sub > j, scaled[0], 0.0)
            lines = [t[j:j+1] * root for t in top]
            top = [jnp.where(sub == j, l, t - below * l) for t, l in zip(top, lines)]
            for r in range(g + 1, depth):
                rows[r] = [x - scaled[r - g] * l for x, l in zip(rows[r], lines)]
            if g + 1 < depth:
                for l in range(8):
                    weight = scaled[1][l:l+1]
                    ahead[l] = [c - s * weight for c, s in zip(ahead[l], scaled[1:])]
        done.append(top)
    return done

def split3(x):
    high = x.astype(jnp.bfloat16)
    low = (x - high.astype(jnp.float32)).astype(jnp.bfloat16)
    return high, low

def cholesky_kernel(scale, panel, gram_ref, out_ref, work, upper):
    size = gram_ref.shape[0]
    tiles = size // LANES
    depth = panel // 8
    work[...] = gram_ref[...] * scale
    upper[...] = jnp.zeros_like(upper)
    dims = (((0,), (0,)), ((), ()))
    for start in range(0, size, panel):
        t0 = start // LANES
        first = start - t0 * LANES
        rows = [[work[start + 8*r : start + 8*r + 8, t*LANES:(t+1)*LANES] for t in range(t0, tiles)] for r in range(depth)]
        done = factor_panel(rows, first)
        full = jnp.concatenate([jnp.concatenate(d, axis=1) for d in done], axis=0)
        row = lax.broadcasted_iota(jnp.int32, full.shape, 0) + first
        col = lax.broadcasted_iota(jnp.int32, full.shape, 1)
        full = jnp.where(row <= col, full, 0.0)
        upper[start:start+panel, t0*LANES:] = full
        stop = start + panel
        if stop == size: break
        high, low = split3(full)
        left = jnp.concatenate([high, high, low], axis=0)
        right = jnp.concatenate([high, low, high], axis=0)
        for t in range(stop // LANES, tiles):
            lo = max(stop, t * LANES)
            off = (t - t0) * LANES
            prod = lax.dot_general(left[:, off:off+LANES], right[:, off:], dims, preferred_element_type=jnp.float32)
            work[lo:(t+1)*LANES, t*LANES:] -= prod[lo - t*LANES:]
    width = out_ref.shape[1]
    if width == size: out_ref[...] = upper[...]
    else: out_ref[...] = upper[:, pl.ds(pl.multiple_of(lax.axis_index("cols") * width, width), width)]

def cholesky(gram, scale, width, panel=32):
    size = gram.shape[0]
    return pl.pallas_call(
        functools.partial(cholesky_kernel, scale, panel),
        out_shape=jax.ShapeDtypeStruct((size, width), jnp.float32),
        in_specs=[pl.BlockSpec(memory_space=pltpu.VMEM)],
        out_specs=pl.BlockSpec(memory_space=pltpu.VMEM),
        scratch_shapes=[pltpu.VMEM((size, size), jnp.float32)] * 2,
    )(gram)


def solution(mesh):
    n, cores = mesh.shape["rows"], mesh.shape["cols"]

    def body(design, signs, kept):
        widths = design.shape[1]
        outgoing = transform(design, signs, kept, design.shape[0] * n)
        sketch, gram = exchange(outgoing, n, cores)
        return (sketch, cholesky(gram, 1.0 / kept.shape[0], widths))

    return jax.shard_map(
        body,
        mesh=mesh,
        in_specs=(P("rows", "cols"), P("rows"), P()),
        out_specs=(P("rows", "cols"), P(None, "cols")),
        check_vma=False,
    )
```

```python
import functools
import math

import jax
import jax.numpy as jnp
from jax import lax
from jax.experimental import pallas as pl
from jax.experimental.pallas import tpu as pltpu
from jax.sharding import PartitionSpec as P

MESH = pl.DeviceIdType.MESH
LANES = 128


def split_two(values):
    high = values.astype(jnp.bfloat16)
    return high, (values - high.astype(jnp.float32)).astype(jnp.bfloat16)


def sketch_kernel(
    low, scale, early,
    design_ref, signs_ref, kept_ref, sketch_ref, gram_ref,
    split, buf, one_a, one_b, out_a, out_b, two_a, two_b, gat,
    one_a_send, one_a_recv, one_b_send, one_b_recv, two_a_send, two_a_recv, two_b_send, two_b_recv,
    az_send, az_recv, axy_send, axy_recv, bxy_send, bxy_recv, bz_send, bz_recv,
    ca_send, ca_recv, cb_send, cb_recv,
):
    me = lax.axis_index("rows")
    core = lax.axis_index("cols")
    high, _, per, width = buf.shape
    length = design_ref.shape[0]
    tile = low * per
    whole = gat.shape[2]
    spot = me % low
    lanes = pl.ds(pl.multiple_of(core * width, LANES), width)
    head, tail = pl.ds(0, early), pl.ds(early, per - early)

    def flip(value, mask):
        bit = 1
        while bit <= mask:
            if mask & bit:
                value = value + (1 - 2 * ((value // bit) % 2)) * bit
            bit *= 2
        return value

    def peer(near, far):
        return flip(me, far * low + near)

    def plane(far):
        return flip(me // low, far)

    def send(src, dst, sems, index, device, other=None):
        return pltpu.make_async_remote_copy(
            src_ref=src, dst_ref=dst, send_sem=sems[0].at[index], recv_sem=sems[1].at[index],
            device_id=(device, core if other is None else other), device_id_type=MESH,
        )

    nears = list(range(low - 1, 0, -1))
    fars = list(range(high - 1, 0, -1))

    barrier = pltpu.get_barrier_semaphore()
    for near in nears:
        pl.semaphore_signal(barrier, inc=1, device_id=(peer(near, 0), core), device_id_type=MESH)
    for far in fars:
        pl.semaphore_signal(barrier, inc=1, device_id=(peer(0, far), core), device_id_type=MESH)
    pl.semaphore_signal(barrier, inc=1, device_id=(me, 1 - core), device_id_type=MESH)

    def one_a_copy(far, near):
        return send(
            buf.at[far, flip(spot, near), head], one_a.at[far, near], (one_a_send, one_a_recv), (far, near),
            peer(near, 0),
        )

    def one_b_copy(far):
        return send(buf.at[far, :, tail], one_b.at[far], (one_b_send, one_b_recv), far, peer(0, far))

    def two_a_copy(far):
        return send(out_a.at[far], two_a.at[far], (two_a_send, two_a_recv), far, peer(0, far))

    def two_b_copy(near):
        return send(
            out_b.at[flip(spot, near)], two_b.at[near], (two_b_send, two_b_recv), near, peer(near, 0)
        )

    def az_copy(far):
        ref = gat.at[me, head, lanes]
        return send(ref, ref, (az_send, az_recv), far, peer(0, far))

    def axy_copy(far, near):
        ref = gat.at[peer(0, far), head, lanes]
        return send(ref, ref, (axy_send, axy_recv), (far, near), peer(near, 0))

    def bxy_copy(near):
        ref = gat.at[me, tail, lanes]
        return send(ref, ref, (bxy_send, bxy_recv), near, peer(near, 0))

    def bz_copy(far):
        ref = gat.at[pl.ds((me // low) * low, low), tail, lanes]
        return send(ref, ref, (bz_send, bz_recv), far, peer(0, far))

    def ca_copy(far, near):
        ref = gat.at[peer(near, far), head, lanes]
        return send(ref, ref, (ca_send, ca_recv), (far, near), me, 1 - core)

    def cb_copy(far):
        ref = gat.at[pl.ds(plane(far) * low, low), tail, lanes]
        return send(ref, ref, (cb_send, cb_recv), far, me, 1 - core)

    split[0], split[1] = split_two(design_ref[...])
    first_row = me * length
    lane = lax.broadcasted_iota(jnp.int32, (LANES, LANES), 1)
    step_rows = min(tile, 256)

    def transform_rows(far, start):
        stacked = []
        for piece in range(step_rows // LANES):
            row = kept_ref[pl.ds(plane(far) * (tile // LANES) + start // LANES + piece, 1), :]
            column = jnp.broadcast_to(row, (LANES, LANES)).T
            blocks = []
            for block in range(length // LANES):
                common = jnp.bitwise_and(column, lane + (first_row + block * LANES))
                odd = jnp.bitwise_and(lax.population_count(common), 1)
                flips = signs_ref[block : block + 1, :]
                entry = (1 - 2 * odd) * flips
                blocks.append(entry.astype(jnp.float32).astype(jnp.bfloat16))
            stacked.append(jnp.concatenate(blocks, axis=1))
        table = jnp.concatenate(stacked, axis=0)
        total = jnp.dot(table, split[1], preferred_element_type=jnp.float32)
        total += jnp.dot(table, split[0], preferred_element_type=jnp.float32)
        owner = start // per
        buf[far, owner : owner + step_rows // per] = (total * scale).reshape(step_rows // per, per, width)

    for far in fars + [0]:
        for start in range(0, tile, step_rows):
            transform_rows(far, start)
        if far == high - 1:
            pl.semaphore_wait(barrier, len(nears) + len(fars) + 1)
        for near in nears:
            one_a_copy(far, near).start()
        if far:
            one_b_copy(far).start()

    def near_sum(far):
        total = buf[far, spot, head]
        for near in nears:
            one_a_copy(far, near).wait_recv()
            total += one_a[far, near]
        return total

    for far in fars:
        out_a[far] = near_sum(far)
        two_a_copy(far).start()
    total = buf[0, :, tail]
    for far in fars:
        one_b_copy(far).wait_recv()
        total += one_b[far]
    out_b[...] = total
    for near in nears:
        two_b_copy(near).start()
    total = near_sum(0)
    for far in fars:
        two_a_copy(far).wait_recv()
        total += two_a[far]
    sketch_ref[head, :] = total
    gat[me, head, lanes] = total
    for far in fars:
        az_copy(far).start()
    for near in nears:
        axy_copy(0, near).start()
    ca_copy(0, 0).start()
    total = out_b[spot]
    for near in nears:
        two_b_copy(near).wait_recv()
        total += two_b[near]
    sketch_ref[tail, :] = total
    gat[me, tail, lanes] = total
    for near in nears:
        bxy_copy(near).start()

    def add_gram(far, first):
        for near in range(low):
            ca_copy(far, near).wait_recv()
        cb_copy(far).wait_recv()
        half = whole // 2
        rows = gat[pl.ds(plane(far) * low, low)].reshape(tile, whole)
        upper, rest = split_two(rows)
        left = jnp.concatenate([upper, upper, rest], axis=0)
        right = jnp.concatenate([upper, rest, upper], axis=0)
        dims = (((0,), (0,)), ((), ()))
        a = lax.dot_general(left[:, :half], right, dims, preferred_element_type=jnp.float32)
        c = lax.dot_general(left[:, half:], right[:, half:], dims, preferred_element_type=jnp.float32)
        gram_ref[0:half, :] = a if first else gram_ref[0:half, :] + a
        gram_ref[half:, half:] = c if first else gram_ref[half:, half:] + c

    for near in nears:
        bxy_copy(near).wait_recv()
    for far in fars:
        bz_copy(far).start()
    cb_copy(0).start()
    for near in nears:
        axy_copy(0, near).wait_recv()
        ca_copy(0, near).start()
    for far in fars:
        az_copy(far).wait_recv()
        for near in nears:
            axy_copy(far, near).start()
        ca_copy(far, 0).start()
    gram_ref[half_rows(gram_ref) :, : whole // 2] = jnp.zeros((whole // 2, whole // 2), jnp.float32)
    add_gram(0, True)
    for far in fars:
        for near in nears:
            axy_copy(far, near).wait_recv()
            ca_copy(far, near).start()
        bz_copy(far).wait_recv()
        cb_copy(far).start()
        add_gram(far, False)

    for far in range(high):
        for near in range(low):
            if near:
                one_a_copy(far, near).wait_send()
                axy_copy(far, near).wait_send()
            ca_copy(far, near).wait_send()
        cb_copy(far).wait_send()
        if far:
            one_b_copy(far).wait_send()
            two_a_copy(far).wait_send()
            az_copy(far).wait_send()
            bz_copy(far).wait_send()
    for near in nears:
        two_b_copy(near).wait_send()
        bxy_copy(near).wait_send()


def half_rows(ref):
    return ref.shape[0] // 2


def sketch_and_gram(design, signs, kept, n, cores):
    length, width = design.shape
    count = kept.shape[0]
    per = count // n
    low = 1 << ((n.bit_length() - 1) // 2)
    high = n // low
    early = per - per // 4
    whole = width * cores
    sems = []
    for shape in ((high, low), (high,), (high,), (low,), (high,), (high, low), (low,), (high,), (high, low), (high,)):
        sems += [pltpu.SemaphoreType.DMA(shape)] * 2
    late = per - early
    return pl.pallas_call(
        functools.partial(sketch_kernel, low, 1.0 / math.sqrt(length * n), early),
        out_shape=(
            jax.ShapeDtypeStruct((per, width), jnp.float32),
            jax.ShapeDtypeStruct((whole, whole), jnp.float32),
        ),
        in_specs=[pl.BlockSpec(memory_space=pltpu.VMEM)] * 3,
        out_specs=(pl.BlockSpec(memory_space=pltpu.VMEM),) * 2,
        scratch_shapes=[
            pltpu.VMEM((2, length, width), jnp.bfloat16),
            pltpu.VMEM((high, low, per, width), jnp.float32),
            pltpu.VMEM((high, low, early, width), jnp.float32),
            pltpu.VMEM((high, low, late, width), jnp.float32),
            pltpu.VMEM((high, early, width), jnp.float32),
            pltpu.VMEM((low, late, width), jnp.float32),
            pltpu.VMEM((high, early, width), jnp.float32),
            pltpu.VMEM((low, late, width), jnp.float32),
            pltpu.VMEM((n, per, whole), jnp.float32),
            *sems,
        ],
        compiler_params=pltpu.CompilerParams(
            collective_id=0, has_side_effects=True, vmem_limit_bytes=60 * 1024 * 1024
        ),
    )(design, signs.reshape(-1, LANES), kept.reshape(-1, LANES))


def spread(x, lane):
    return jnp.broadcast_to(x[:, lane:lane+1], x.shape)

def factor_panel(rows, first):
    depth = len(rows)
    tiles = len(rows[0])
    sub = lax.broadcasted_iota(jnp.int32, (8, LANES), 0)
    rows = [list(r) for r in rows]
    ahead = [[spread(rows[r][0], first + j) for r in range(depth)] for j in range(8)]
    done = []
    for g in range(depth):
        here = ahead
        if g + 1 < depth:
            ahead = [[spread(rows[r][0], first + 8 * (g + 1) + j) for r in range(g + 1, depth)] for j in range(8)]
        top = rows[g]
        for j in range(8):
            column = here[j]
            root = lax.rsqrt(column[0][j:j+1])
            root = jnp.broadcast_to(root, (8, LANES))
            scaled = [c * root for c in column]
            for later in range(j + 1, 8):
                weight = here[later][0][j:j+1] * root
                here[later] = [c - s * weight for c, s in zip(here[later], scaled)]
            below = jnp.where(sub > j, scaled[0], 0.0)
            lines = [t[j:j+1] * root for t in top]
            top = [jnp.where(sub == j, l, t - below * l) for t, l in zip(top, lines)]
            for r in range(g + 1, depth):
                rows[r] = [x - scaled[r - g] * l for x, l in zip(rows[r], lines)]
            if g + 1 < depth:
                for l in range(8):
                    weight = scaled[1][l:l+1]
                    ahead[l] = [c - s * weight for c, s in zip(ahead[l], scaled[1:])]
        done.append(top)
    return done

def cholesky_kernel(scale, panel, gram_ref, out_ref, work, upper):
    size = gram_ref.shape[0]
    tiles = size // LANES
    depth = panel // 8
    work[...] = gram_ref[...] * scale
    upper[...] = jnp.zeros_like(upper)
    dims = (((0,), (0,)), ((), ()))
    for start in range(0, size, panel):
        t0 = start // LANES
        first = start - t0 * LANES
        rows = [[work[start + 8*r : start + 8*r + 8, t*LANES:(t+1)*LANES] for t in range(t0, tiles)] for r in range(depth)]
        done = factor_panel(rows, first)
        full = jnp.concatenate([jnp.concatenate(d, axis=1) for d in done], axis=0)
        row = lax.broadcasted_iota(jnp.int32, full.shape, 0) + first
        col = lax.broadcasted_iota(jnp.int32, full.shape, 1)
        full = jnp.where(row <= col, full, 0.0)
        upper[start:start+panel, t0*LANES:] = full
        stop = start + panel
        if stop == size: break
        high, low = split_two(full)
        left = jnp.concatenate([high, high, low], axis=0)
        right = jnp.concatenate([high, low, high], axis=0)
        for t in range(stop // LANES, tiles):
            lo = max(stop, t * LANES)
            off = (t - t0) * LANES
            prod = lax.dot_general(left[:, off:off+LANES], right[:, off:], dims, preferred_element_type=jnp.float32)
            work[lo:(t+1)*LANES, t*LANES:] -= prod[lo - t*LANES:]
    width = out_ref.shape[1]
    if width == size: out_ref[...] = upper[...]
    else: out_ref[...] = upper[:, pl.ds(pl.multiple_of(lax.axis_index("cols") * width, width), width)]

def cholesky(gram, scale, width, panel=32):
    size = gram.shape[0]
    return pl.pallas_call(
        functools.partial(cholesky_kernel, scale, panel),
        out_shape=jax.ShapeDtypeStruct((size, width), jnp.float32),
        in_specs=[pl.BlockSpec(memory_space=pltpu.VMEM)],
        out_specs=pl.BlockSpec(memory_space=pltpu.VMEM),
        scratch_shapes=[pltpu.VMEM((size, size), jnp.float32)] * 2,
    )(gram)


def solution(mesh):
    n, cores = mesh.shape["rows"], mesh.shape["cols"]

    def body(design, signs, kept):
        sketch, gram = sketch_and_gram(design, signs, kept, n, cores)
        return (sketch, cholesky(gram, 1.0 / kept.shape[0], design.shape[1]))

    return jax.shard_map(
        body,
        mesh=mesh,
        in_specs=(P("rows", "cols"), P("rows"), P()),
        out_specs=(P("rows", "cols"), P(None, "cols")),
        check_vma=False,
    )
```

```python
import functools
import math

import jax
import jax.numpy as jnp
from jax import lax
from jax.experimental import pallas as pl
from jax.experimental.pallas import tpu as pltpu
from jax.sharding import PartitionSpec as P

MESH = pl.DeviceIdType.MESH
LANES = 128
LOADS = 2


def split_two(values):
    high = values.astype(jnp.bfloat16)
    return high, (values - high.astype(jnp.float32)).astype(jnp.bfloat16)


def sketch_kernel(
    low, scale, early,
    design_hbm, signs_hbm, kept_hbm, sketch_ref, gram_ref,
    design_ref, signs_ref, kept_ref, load_sems, split, buf, one_a, one_b, out_a, out_b, two_a, two_b, gat,
    one_a_send, one_a_recv, one_b_send, one_b_recv, two_a_send, two_a_recv, two_b_send, two_b_recv,
    az_send, az_recv, axy_send, axy_recv, bxy_send, bxy_recv, bz_send, bz_recv,
    ca_send, ca_recv, cb_send, cb_recv,
):
    me = lax.axis_index("rows")
    core = lax.axis_index("cols")
    high, _, per, width = buf.shape
    loads = [
        pltpu.make_async_copy(kept_hbm, kept_ref, load_sems.at[0]),
        pltpu.make_async_copy(signs_hbm, signs_ref, load_sems.at[1]),
    ]
    chunk = design_ref.shape[0] // LOADS
    for index in range(LOADS):
        piece = pl.ds(index * chunk, chunk)
        loads.append(
            pltpu.make_async_copy(design_hbm.at[piece], design_ref.at[piece], load_sems.at[2 + index])
        )
    for load in loads:
        load.start()
    length = design_ref.shape[0]
    tile = low * per
    whole = gat.shape[2]
    spot = me % low
    lanes = pl.ds(pl.multiple_of(core * width, LANES), width)
    head, tail = pl.ds(0, early), pl.ds(early, per - early)

    def flip(value, mask):
        bit = 1
        while bit <= mask:
            if mask & bit:
                value = value + (1 - 2 * ((value // bit) % 2)) * bit
            bit *= 2
        return value

    def peer(near, far):
        return flip(me, far * low + near)

    def plane(far):
        return flip(me // low, far)

    def send(src, dst, sems, index, device, other=None):
        return pltpu.make_async_remote_copy(
            src_ref=src, dst_ref=dst, send_sem=sems[0].at[index], recv_sem=sems[1].at[index],
            device_id=(device, core if other is None else other), device_id_type=MESH,
        )

    nears = list(range(low - 1, 0, -1))
    fars = list(range(high - 1, 0, -1))

    barrier = pltpu.get_barrier_semaphore()
    for near in nears:
        pl.semaphore_signal(barrier, inc=1, device_id=(peer(near, 0), core), device_id_type=MESH)
    for far in fars:
        pl.semaphore_signal(barrier, inc=1, device_id=(peer(0, far), core), device_id_type=MESH)
    pl.semaphore_signal(barrier, inc=1, device_id=(me, 1 - core), device_id_type=MESH)

    def one_a_copy(far, near):
        return send(
            buf.at[far, flip(spot, near), head], one_a.at[far, near], (one_a_send, one_a_recv), (far, near),
            peer(near, 0),
        )

    def one_b_copy(far):
        return send(buf.at[far, :, tail], one_b.at[far], (one_b_send, one_b_recv), far, peer(0, far))

    def two_a_copy(far):
        return send(out_a.at[far], two_a.at[far], (two_a_send, two_a_recv), far, peer(0, far))

    def two_b_copy(near):
        return send(
            out_b.at[flip(spot, near)], two_b.at[near], (two_b_send, two_b_recv), near, peer(near, 0)
        )

    def az_copy(far):
        ref = gat.at[me, head, lanes]
        return send(ref, ref, (az_send, az_recv), far, peer(0, far))

    def axy_copy(far, near):
        ref = gat.at[peer(0, far), head, lanes]
        return send(ref, ref, (axy_send, axy_recv), (far, near), peer(near, 0))

    def bxy_copy(near):
        ref = gat.at[me, tail, lanes]
        return send(ref, ref, (bxy_send, bxy_recv), near, peer(near, 0))

    def bz_copy(far):
        ref = gat.at[pl.ds((me // low) * low, low), tail, lanes]
        return send(ref, ref, (bz_send, bz_recv), far, peer(0, far))

    def ca_copy(far, near):
        ref = gat.at[peer(near, far), head, lanes]
        return send(ref, ref, (ca_send, ca_recv), (far, near), me, 1 - core)

    def cb_copy(far):
        ref = gat.at[pl.ds(plane(far) * low, low), tail, lanes]
        return send(ref, ref, (cb_send, cb_recv), far, me, 1 - core)

    first_row = me * length
    lane = lax.broadcasted_iota(jnp.int32, (LANES, LANES), 1)
    step_rows = min(tile, 256)

    def transform_rows(far, start):
        stacked = []
        for piece in range(step_rows // LANES):
            row = kept_ref[pl.ds(plane(far) * (tile // LANES) + start // LANES + piece, 1), :]
            column = jnp.broadcast_to(row, (LANES, LANES)).T
            blocks = []
            for block in range(length // LANES):
                common = jnp.bitwise_and(column, lane + (first_row + block * LANES))
                odd = jnp.bitwise_and(lax.population_count(common), 1)
                flips = signs_ref[block : block + 1, :]
                entry = (1 - 2 * odd) * flips
                blocks.append(entry.astype(jnp.float32).astype(jnp.bfloat16))
            stacked.append(jnp.concatenate(blocks, axis=1))
        table = jnp.concatenate(stacked, axis=0)
        if far == high - 1 and start == 0:
            for index in range(LOADS):
                loads[2 + index].wait()
                piece = slice(index * chunk, (index + 1) * chunk)
                split[0, piece], split[1, piece] = split_two(design_ref[piece])
        total = jnp.dot(table, split[1], preferred_element_type=jnp.float32)
        total += jnp.dot(table, split[0], preferred_element_type=jnp.float32)
        owner = start // per
        buf[far, owner : owner + step_rows // per] = (total * scale).reshape(step_rows // per, per, width)

    loads[0].wait()
    loads[1].wait()
    for far in fars + [0]:
        for start in range(0, tile, step_rows):
            transform_rows(far, start)
        if far == high - 1:
            pl.semaphore_wait(barrier, len(nears) + len(fars) + 1)
        for near in nears:
            one_a_copy(far, near).start()
        if far:
            one_b_copy(far).start()

    def near_sum(far):
        total = buf[far, spot, head]
        for near in nears:
            one_a_copy(far, near).wait_recv()
            total += one_a[far, near]
        return total

    for far in fars:
        out_a[far] = near_sum(far)
        two_a_copy(far).start()
    total = buf[0, :, tail]
    for far in fars:
        one_b_copy(far).wait_recv()
        total += one_b[far]
    out_b[...] = total
    for near in nears:
        two_b_copy(near).start()
    total = near_sum(0)
    for far in fars:
        two_a_copy(far).wait_recv()
        total += two_a[far]
    sketch_ref[head, :] = total
    gat[me, head, lanes] = total
    for far in fars:
        az_copy(far).start()
    for near in nears:
        axy_copy(0, near).start()
    ca_copy(0, 0).start()
    total = out_b[spot]
    for near in nears:
        two_b_copy(near).wait_recv()
        total += two_b[near]
    sketch_ref[tail, :] = total
    gat[me, tail, lanes] = total
    for near in nears:
        bxy_copy(near).start()

    def add_gram(far, first):
        for near in range(low):
            ca_copy(far, near).wait_recv()
        cb_copy(far).wait_recv()
        half = whole // 2
        rows = gat[pl.ds(plane(far) * low, low)].reshape(tile, whole)
        upper, rest = split_two(rows)
        left = jnp.concatenate([upper, upper, rest], axis=0)
        right = jnp.concatenate([upper, rest, upper], axis=0)
        dims = (((0,), (0,)), ((), ()))
        a = lax.dot_general(left[:, :half], right, dims, preferred_element_type=jnp.float32)
        c = lax.dot_general(left[:, half:], right[:, half:], dims, preferred_element_type=jnp.float32)
        gram_ref[0:half, :] = a if first else gram_ref[0:half, :] + a
        gram_ref[half:, half:] = c if first else gram_ref[half:, half:] + c

    for near in nears:
        bxy_copy(near).wait_recv()
    for far in fars:
        bz_copy(far).start()
    cb_copy(0).start()
    for near in nears:
        axy_copy(0, near).wait_recv()
        ca_copy(0, near).start()
    for far in fars:
        az_copy(far).wait_recv()
        for near in nears:
            axy_copy(far, near).start()
        ca_copy(far, 0).start()
    gram_ref[half_rows(gram_ref) :, : whole // 2] = jnp.zeros((whole // 2, whole // 2), jnp.float32)
    add_gram(0, True)
    for far in fars:
        for near in nears:
            axy_copy(far, near).wait_recv()
            ca_copy(far, near).start()
        bz_copy(far).wait_recv()
        cb_copy(far).start()
        add_gram(far, False)

    for far in range(high):
        for near in range(low):
            if near:
                one_a_copy(far, near).wait_send()
                axy_copy(far, near).wait_send()
            ca_copy(far, near).wait_send()
        cb_copy(far).wait_send()
        if far:
            one_b_copy(far).wait_send()
            two_a_copy(far).wait_send()
            az_copy(far).wait_send()
            bz_copy(far).wait_send()
    for near in nears:
        two_b_copy(near).wait_send()
        bxy_copy(near).wait_send()


def half_rows(ref):
    return ref.shape[0] // 2


def sketch_and_gram(design, signs, kept, n, cores):
    length, width = design.shape
    count = kept.shape[0]
    per = count // n
    low = 1 << ((n.bit_length() - 1) // 2)
    high = n // low
    early = per - per // 4
    whole = width * cores
    sems = []
    for shape in ((high, low), (high,), (high,), (low,), (high,), (high, low), (low,), (high,), (high, low), (high,)):
        sems += [pltpu.SemaphoreType.DMA(shape)] * 2
    late = per - early
    limit = min(60 * 1024 * 1024, 4 * (7 * count * width + 3 * length * width + whole * whole) + 12 * 1024 * 1024)
    return pl.pallas_call(
        functools.partial(sketch_kernel, low, 1.0 / math.sqrt(length * n), early),
        out_shape=(
            jax.ShapeDtypeStruct((per, width), jnp.float32),
            jax.ShapeDtypeStruct((whole, whole), jnp.float32),
        ),
        in_specs=[pl.BlockSpec(memory_space=pltpu.HBM)] * 3,
        out_specs=(pl.BlockSpec(memory_space=pltpu.VMEM),) * 2,
        scratch_shapes=[
            pltpu.VMEM((length, width), jnp.float32),
            pltpu.VMEM((length // LANES, LANES), jnp.int32),
            pltpu.VMEM((count // LANES, LANES), jnp.int32),
            pltpu.SemaphoreType.DMA((2 + LOADS,)),
            pltpu.VMEM((2, length, width), jnp.bfloat16),
            pltpu.VMEM((high, low, per, width), jnp.float32),
            pltpu.VMEM((high, low, early, width), jnp.float32),
            pltpu.VMEM((high, low, late, width), jnp.float32),
            pltpu.VMEM((high, early, width), jnp.float32),
            pltpu.VMEM((low, late, width), jnp.float32),
            pltpu.VMEM((high, early, width), jnp.float32),
            pltpu.VMEM((low, late, width), jnp.float32),
            pltpu.VMEM((n, per, whole), jnp.float32),
            *sems,
        ],
        compiler_params=pltpu.CompilerParams(
            collective_id=0, has_side_effects=True, vmem_limit_bytes=limit
        ),
    )(*(pltpu.with_memory_space_constraint(x, pltpu.HBM) for x in (design, signs.reshape(-1, LANES), kept.reshape(-1, LANES))))


def spread(x, lane):
    return jnp.broadcast_to(x[:, lane:lane+1], x.shape)

def factor_panel(rows, first):
    depth = len(rows)
    tiles = len(rows[0])
    sub = lax.broadcasted_iota(jnp.int32, (8, LANES), 0)
    rows = [list(r) for r in rows]
    ahead = [[spread(rows[r][0], first + j) for r in range(depth)] for j in range(8)]
    done = []
    for g in range(depth):
        here = ahead
        if g + 1 < depth:
            ahead = [[spread(rows[r][0], first + 8 * (g + 1) + j) for r in range(g + 1, depth)] for j in range(8)]
        top = rows[g]
        for j in range(8):
            column = here[j]
            root = lax.rsqrt(column[0][j:j+1])
            root = jnp.broadcast_to(root, (8, LANES))
            scaled = [c * root for c in column]
            for later in range(j + 1, 8):
                weight = here[later][0][j:j+1] * root
                here[later] = [c - s * weight for c, s in zip(here[later], scaled)]
            below = jnp.where(sub > j, scaled[0], 0.0)
            lines = [t[j:j+1] * root for t in top]
            top = [jnp.where(sub == j, l, t - below * l) for t, l in zip(top, lines)]
            for r in range(g + 1, depth):
                rows[r] = [x - scaled[r - g] * l for x, l in zip(rows[r], lines)]
            if g + 1 < depth:
                for l in range(8):
                    weight = scaled[1][l:l+1]
                    ahead[l] = [c - s * weight for c, s in zip(ahead[l], scaled[1:])]
        done.append(top)
    return done

def cholesky_kernel(scale, panel, gram_ref, sketch_ref, sketch_hbm, out_hbm, work, upper, sems):
    size = gram_ref.shape[0]
    width = out_hbm.shape[1]
    tiles = size // LANES
    depth = panel // 8
    lanes = pl.ds(pl.multiple_of(lax.axis_index("cols") * width, width), width)
    copies = [pltpu.make_async_copy(sketch_ref, sketch_hbm, sems.at[size // panel])]
    copies[0].start()
    work[...] = gram_ref[...] * scale
    dims = (((0,), (0,)), ((), ()))
    for start in range(0, size, panel):
        base = start // LANES
        first = start - base * LANES
        rows = [
            [
                work[start + 8 * r : start + 8 * r + 8, t * LANES : (t + 1) * LANES]
                for t in range(base, tiles)
            ]
            for r in range(depth)
        ]
        done = factor_panel(rows, first)
        full = jnp.concatenate([jnp.concatenate(d, axis=1) for d in done], axis=0)
        row = lax.broadcasted_iota(jnp.int32, full.shape, 0) + first
        column = lax.broadcasted_iota(jnp.int32, full.shape, 1)
        full = jnp.where(row <= column, full, 0.0)
        stop = start + panel
        if base:
            upper[start:stop, : base * LANES] = jnp.zeros((panel, base * LANES), jnp.float32)
        upper[start:stop, base * LANES :] = full
        copies.append(
            pltpu.make_async_copy(
                upper.at[start:stop, lanes], out_hbm.at[start:stop], sems.at[start // panel]
            )
        )
        copies[-1].start()
        if stop == size:
            break
        high, low = split_two(full)
        left = jnp.concatenate([high, high, low], axis=0)
        right = jnp.concatenate([high, low, high], axis=0)
        for t in range(stop // LANES, tiles):
            begin = max(stop, t * LANES)
            offset = (t - base) * LANES
            product = lax.dot_general(
                left[:, offset : offset + LANES], right[:, offset:], dims, preferred_element_type=jnp.float32
            )
            work[begin : (t + 1) * LANES, t * LANES :] -= product[begin - t * LANES :]
    for copy in copies:
        copy.wait()


def cholesky(gram, sketch, scale, width, panel=32):
    size = gram.shape[0]
    return pl.pallas_call(
        functools.partial(cholesky_kernel, scale, panel),
        out_shape=(
            jax.ShapeDtypeStruct(sketch.shape, jnp.float32),
            jax.ShapeDtypeStruct((size, width), jnp.float32),
        ),
        in_specs=[pl.BlockSpec(memory_space=pltpu.VMEM)] * 2,
        out_specs=(pl.BlockSpec(memory_space=pltpu.HBM),) * 2,
        scratch_shapes=[
            pltpu.VMEM((size, size), jnp.float32),
            pltpu.VMEM((size, size), jnp.float32),
            pltpu.SemaphoreType.DMA((size // panel + 1,)),
        ],
        compiler_params=pltpu.CompilerParams(vmem_limit_bytes=16 * 1024 * 1024),
    )(gram, sketch)


def solution(mesh):
    n, cores = mesh.shape["rows"], mesh.shape["cols"]

    def body(design, signs, kept):
        sketch, gram = sketch_and_gram(design, signs, kept, n, cores)
        return cholesky(gram, sketch, 1.0 / kept.shape[0], design.shape[1])

    return jax.shard_map(
        body,
        mesh=mesh,
        in_specs=(P("rows", "cols"), P("rows"), P()),
        out_specs=(P("rows", "cols"), P(None, "cols")),
        check_vma=False,
    )
```

```python
import functools
import math

import jax
import jax.numpy as jnp
from jax import lax
from jax.experimental import pallas as pl
from jax.experimental.pallas import tpu as pltpu
from jax.sharding import PartitionSpec as P

MESH = pl.DeviceIdType.MESH
LANES = 128
LOADS = 2


def split_two(values):
    high = values.astype(jnp.bfloat16)
    return high, (values - high.astype(jnp.float32)).astype(jnp.bfloat16)


def sketch_kernel(
    low, scale, early, gathers,
    design_hbm, signs_hbm, kept_hbm, sketch_ref, gram_ref,
    design_ref, signs_ref, kept_ref, load_sems, split, buf, one_a, one_b, out_a, out_b, two_a, two_b, gat,
    one_a_send, one_a_recv, one_b_send, one_b_recv, two_a_send, two_a_recv, two_b_send, two_b_recv,
    far_send, far_recv, near_send, near_recv, core_send, core_recv,
):
    me = lax.axis_index("rows")
    core = lax.axis_index("cols")
    high, _, per, width = buf.shape
    loads = [
        pltpu.make_async_copy(kept_hbm, kept_ref, load_sems.at[0]),
        pltpu.make_async_copy(signs_hbm, signs_ref, load_sems.at[1]),
    ]
    chunk = design_ref.shape[0] // LOADS
    for index in range(LOADS):
        piece = pl.ds(index * chunk, chunk)
        loads.append(
            pltpu.make_async_copy(design_hbm.at[piece], design_ref.at[piece], load_sems.at[2 + index])
        )
    for load in loads:
        load.start()
    length = design_ref.shape[0]
    tile = low * per
    whole = gat.shape[2]
    spot = me % low
    lanes = pl.ds(pl.multiple_of(core * width, LANES), width)
    head, tail = pl.ds(0, early), pl.ds(early, per - early)

    def flip(value, mask):
        bit = 1
        while bit <= mask:
            if mask & bit:
                value = value + (1 - 2 * ((value // bit) % 2)) * bit
            bit *= 2
        return value

    def peer(near, far):
        return flip(me, far * low + near)

    def plane(far):
        return flip(me // low, far)

    def send(src, dst, sems, index, device, other=None):
        return pltpu.make_async_remote_copy(
            src_ref=src, dst_ref=dst, send_sem=sems[0].at[index], recv_sem=sems[1].at[index],
            device_id=(device, core if other is None else other), device_id_type=MESH,
        )

    nears = list(range(low - 1, 0, -1))
    fars = list(range(high - 1, 0, -1))
    closest = sorted(fars, key=lambda far: far > 1)

    barrier = pltpu.get_barrier_semaphore()
    for near in nears:
        pl.semaphore_signal(barrier, inc=1, device_id=(peer(near, 0), core), device_id_type=MESH)
    for far in fars:
        pl.semaphore_signal(barrier, inc=1, device_id=(peer(0, far), core), device_id_type=MESH)
    pl.semaphore_signal(barrier, inc=1, device_id=(me, 1 - core), device_id_type=MESH)

    def one_a_copy(far, near):
        return send(
            buf.at[far, flip(spot, near), head], one_a.at[far, near], (one_a_send, one_a_recv), (far, near),
            peer(near, 0),
        )

    def one_b_copy(far):
        return send(buf.at[far, :, tail], one_b.at[far], (one_b_send, one_b_recv), far, peer(0, far))

    def two_a_copy(far):
        return send(out_a.at[far], two_a.at[far], (two_a_send, two_a_recv), far, peer(0, far))

    def two_b_copy(near):
        return send(
            out_b.at[flip(spot, near)], two_b.at[near], (two_b_send, two_b_recv), near, peer(near, 0)
        )

    def rows_of(part):
        return pl.ds(gathers[part][1], gathers[part][2])

    def near_copy(part, far, near):
        ref = gat.at[peer(0, far), rows_of(part), lanes]
        return send(ref, ref, (near_send, near_recv), (part, far, near), peer(near, 0))

    def far_copy(part, far):
        if gathers[part][0]:
            ref = gat.at[me, rows_of(part), lanes]
        else:
            ref = gat.at[pl.ds((me // low) * low, low), rows_of(part), lanes]
        return send(ref, ref, (far_send, far_recv), (part, far), peer(0, far))

    def core_copy(part, far):
        ref = gat.at[pl.ds(plane(far) * low, low), rows_of(part), lanes]
        return send(ref, ref, (core_send, core_recv), (part, far), me, 1 - core)

    def begin(part):
        if gathers[part][0]:
            for far in closest:
                far_copy(part, far).start()
        for near in nears:
            near_copy(part, 0, near).start()

    def middle(part, far):
        if gathers[part][0]:
            far_copy(part, far).wait_recv()
            for near in nears:
                near_copy(part, far, near).start()
        else:
            for near in nears:
                near_copy(part, 0, near).wait_recv()
            for other in fars:
                far_copy(part, other).start()
            core_copy(part, 0).start()

    def finish(part, far):
        if gathers[part][0]:
            for near in nears:
                near_copy(part, far, near).wait_recv()
        else:
            far_copy(part, far).wait_recv()
        core_copy(part, far).start()

    first_row = me * length
    lane = lax.broadcasted_iota(jnp.int32, (LANES, LANES), 1)
    step_rows = min(tile, 256)

    def transform_rows(far, start):
        stacked = []
        for piece in range(step_rows // LANES):
            row = kept_ref[pl.ds(plane(far) * (tile // LANES) + start // LANES + piece, 1), :]
            column = jnp.broadcast_to(row, (LANES, LANES)).T
            blocks = []
            for block in range(length // LANES):
                common = jnp.bitwise_and(column, lane + (first_row + block * LANES))
                odd = jnp.bitwise_and(lax.population_count(common), 1)
                flips = signs_ref[block : block + 1, :]
                entry = (1 - 2 * odd) * flips
                blocks.append(entry.astype(jnp.float32).astype(jnp.bfloat16))
            stacked.append(jnp.concatenate(blocks, axis=1))
        table = jnp.concatenate(stacked, axis=0)
        if far == high - 1 and start == 0:
            for index in range(LOADS):
                loads[2 + index].wait()
                piece = slice(index * chunk, (index + 1) * chunk)
                split[0, piece], split[1, piece] = split_two(design_ref[piece])
        total = jnp.dot(table, split[1], preferred_element_type=jnp.float32)
        total += jnp.dot(table, split[0], preferred_element_type=jnp.float32)
        owner = start // per
        buf[far, owner : owner + step_rows // per] = (total * scale).reshape(step_rows // per, per, width)

    loads[0].wait()
    loads[1].wait()
    for far in fars + [0]:
        for start in range(0, tile, step_rows):
            transform_rows(far, start)
        if far == high - 1:
            pl.semaphore_wait(barrier, len(nears) + len(fars) + 1)
        for near in nears:
            one_a_copy(far, near).start()
        if far:
            one_b_copy(far).start()

    def near_sum(far):
        total = buf[far, spot, head]
        for near in nears:
            one_a_copy(far, near).wait_recv()
            total += one_a[far, near]
        return total

    for far in fars:
        out_a[far] = near_sum(far)
        two_a_copy(far).start()
    total = buf[0, :, tail]
    for far in fars:
        one_b_copy(far).wait_recv()
        total += one_b[far]
    out_b[...] = total
    for near in nears:
        two_b_copy(near).start()
    total = near_sum(0)
    for far in fars:
        two_a_copy(far).wait_recv()
        total += two_a[far]
    sketch_ref[head, :] = total
    gat[me, head, lanes] = total
    for part in [part for part in range(len(gathers)) if gathers[part][1] < early]:
        begin(part)
    total = out_b[spot]
    for near in nears:
        two_b_copy(near).wait_recv()
        total += two_b[near]
    sketch_ref[tail, :] = total
    gat[me, tail, lanes] = total
    for part in [part for part in range(len(gathers)) if gathers[part][1] >= early]:
        begin(part)

    def add_gram(far, first):
        for part in range(len(gathers)):
            core_copy(part, far).wait_recv()
        half = whole // 2
        rows = gat[pl.ds(plane(far) * low, low)].reshape(tile, whole)
        upper, rest = split_two(rows)
        left = jnp.concatenate([upper, upper, rest], axis=0)
        right = jnp.concatenate([upper, rest, upper], axis=0)
        dims = (((0,), (0,)), ((), ()))
        a = lax.dot_general(left[:, :half], right, dims, preferred_element_type=jnp.float32)
        c = lax.dot_general(left[:, half:], right[:, half:], dims, preferred_element_type=jnp.float32)
        gram_ref[0:half, :] = a if first else gram_ref[0:half, :] + a
        gram_ref[half:, half:] = c if first else gram_ref[half:, half:] + c

    passed = [part for part in range(len(gathers)) if gathers[part][0]]
    for part in range(len(gathers)):
        if part not in passed:
            middle(part, 0)
    for index, far in enumerate(closest):
        for part in passed:
            middle(part, far)
            if index == 0:
                finish(part, 0)
    gram_ref[half_rows(gram_ref) :, : whole // 2] = jnp.zeros((whole // 2, whole // 2), jnp.float32)
    ready = 0
    for far in closest:
        for part in range(len(gathers)):
            finish(part, far)
        add_gram(ready, ready == 0)
        ready = far
    add_gram(ready, ready == 0)

    for far in range(high):
        for near in nears:
            one_a_copy(far, near).wait_send()
        if far:
            one_b_copy(far).wait_send()
            two_a_copy(far).wait_send()
        for part in range(len(gathers)):
            core_copy(part, far).wait_send()
            if far:
                far_copy(part, far).wait_send()
            if gathers[part][0] or far == 0:
                for near in nears:
                    near_copy(part, far, near).wait_send()
    for near in nears:
        two_b_copy(near).wait_send()


def half_rows(ref):
    return ref.shape[0] // 2


def sketch_and_gram(design, signs, kept, n, cores):
    length, width = design.shape
    count = kept.shape[0]
    per = count // n
    low = 1 << ((n.bit_length() - 1) // 2)
    high = n // low
    early = per - per // 4
    eighth = per // 8
    gathers = ((0, 0, eighth), (1, eighth, early - eighth), (1, early, per - early))
    whole = width * cores
    sems = []
    count_g = len(gathers)
    for shape in ((high, low), (high,), (high,), (low,), (count_g, high), (count_g, high, low), (count_g, high)):
        sems += [pltpu.SemaphoreType.DMA(shape)] * 2
    late = per - early
    limit = min(60 * 1024 * 1024, 4 * (7 * count * width + 3 * length * width + whole * whole) + 12 * 1024 * 1024)
    return pl.pallas_call(
        functools.partial(sketch_kernel, low, 1.0 / math.sqrt(length * n), early, gathers),
        out_shape=(
            jax.ShapeDtypeStruct((per, width), jnp.float32),
            jax.ShapeDtypeStruct((whole, whole), jnp.float32),
        ),
        in_specs=[pl.BlockSpec(memory_space=pltpu.HBM)] * 3,
        out_specs=(pl.BlockSpec(memory_space=pltpu.VMEM),) * 2,
        scratch_shapes=[
            pltpu.VMEM((length, width), jnp.float32),
            pltpu.VMEM((length // LANES, LANES), jnp.int32),
            pltpu.VMEM((count // LANES, LANES), jnp.int32),
            pltpu.SemaphoreType.DMA((2 + LOADS,)),
            pltpu.VMEM((2, length, width), jnp.bfloat16),
            pltpu.VMEM((high, low, per, width), jnp.float32),
            pltpu.VMEM((high, low, early, width), jnp.float32),
            pltpu.VMEM((high, low, late, width), jnp.float32),
            pltpu.VMEM((high, early, width), jnp.float32),
            pltpu.VMEM((low, late, width), jnp.float32),
            pltpu.VMEM((high, early, width), jnp.float32),
            pltpu.VMEM((low, late, width), jnp.float32),
            pltpu.VMEM((n, per, whole), jnp.float32),
            *sems,
        ],
        compiler_params=pltpu.CompilerParams(
            collective_id=0, has_side_effects=True, vmem_limit_bytes=limit
        ),
    )(*(pltpu.with_memory_space_constraint(x, pltpu.HBM) for x in (design, signs.reshape(-1, LANES), kept.reshape(-1, LANES))))


def spread(x, lane):
    return jnp.broadcast_to(x[:, lane:lane+1], x.shape)

def factor_panel(rows, first, reach):
    depth = len(rows)
    size = 8 * depth
    sub = lax.broadcasted_iota(jnp.int32, (8, LANES), 0)
    rows = [list(r) for r in rows]
    columns = {}

    def fetch(j):
        if j < size:
            columns[j] = [spread(rows[r][0], first + j) for r in range(j // 8, depth)]

    for j in range(reach + 1):
        fetch(j)
    for i in range(size):
        g, j = i // 8, i % 8
        column = columns.pop(i)
        root = jnp.broadcast_to(lax.rsqrt(column[0][j : j + 1]), (8, LANES))
        scaled = [c * root for c in column]
        for later in range(i + 1, min(i + reach, size - 1) + 1):
            q = later // 8
            if q == g and later == i + 1:
                weight = columns[later][0][j : j + 1] * root
            else:
                weight = scaled[q - g][later % 8 : later % 8 + 1]
            columns[later] = [c - s * weight for c, s in zip(columns[later], scaled[q - g :])]
        below = jnp.where(sub > j, scaled[0], 0.0)
        lines = [t[j : j + 1] * root for t in rows[g]]
        rows[g] = [jnp.where(sub == j, l, t - below * l) for t, l in zip(rows[g], lines)]
        for r in range(g + 1, depth):
            rows[r] = [x - scaled[r - g] * l for x, l in zip(rows[r], lines)]
        fetch(i + reach + 1)
    return rows


def cholesky_kernel(scale, panel, reach, gram_ref, sketch_ref, sketch_hbm, out_hbm, work, upper, sems):
    size = gram_ref.shape[0]
    width = out_hbm.shape[1]
    tiles = size // LANES
    depth = panel // 8
    lanes = pl.ds(pl.multiple_of(lax.axis_index("cols") * width, width), width)
    copies = [pltpu.make_async_copy(sketch_ref, sketch_hbm, sems.at[size // panel])]
    copies[0].start()
    work[...] = gram_ref[...] * scale
    dims = (((0,), (0,)), ((), ()))
    for start in range(0, size, panel):
        base = start // LANES
        first = start - base * LANES
        rows = [
            [
                work[start + 8 * r : start + 8 * r + 8, t * LANES : (t + 1) * LANES]
                for t in range(base, tiles)
            ]
            for r in range(depth)
        ]
        done = factor_panel(rows, first, reach)
        full = jnp.concatenate([jnp.concatenate(d, axis=1) for d in done], axis=0)
        row = lax.broadcasted_iota(jnp.int32, full.shape, 0) + first
        column = lax.broadcasted_iota(jnp.int32, full.shape, 1)
        full = jnp.where(row <= column, full, 0.0)
        stop = start + panel
        if base:
            upper[start:stop, : base * LANES] = jnp.zeros((panel, base * LANES), jnp.float32)
        upper[start:stop, base * LANES :] = full
        copies.append(
            pltpu.make_async_copy(
                upper.at[start:stop, lanes], out_hbm.at[start:stop], sems.at[start // panel]
            )
        )
        copies[-1].start()
        if stop == size:
            break
        high, low = split_two(full)
        left = jnp.concatenate([high, high, low], axis=0)
        right = jnp.concatenate([high, low, high], axis=0)
        for t in range(stop // LANES, tiles):
            begin = max(stop, t * LANES)
            offset = (t - base) * LANES
            product = lax.dot_general(
                left[:, offset : offset + LANES], right[:, offset:], dims, preferred_element_type=jnp.float32
            )
            work[begin : (t + 1) * LANES, t * LANES :] -= product[begin - t * LANES :]
    for copy in copies:
        copy.wait()


def cholesky(gram, sketch, scale, width, panel=32, reach=12):
    size = gram.shape[0]
    return pl.pallas_call(
        functools.partial(cholesky_kernel, scale, panel, reach),
        out_shape=(
            jax.ShapeDtypeStruct(sketch.shape, jnp.float32),
            jax.ShapeDtypeStruct((size, width), jnp.float32),
        ),
        in_specs=[pl.BlockSpec(memory_space=pltpu.VMEM)] * 2,
        out_specs=(pl.BlockSpec(memory_space=pltpu.HBM),) * 2,
        scratch_shapes=[
            pltpu.VMEM((size, size), jnp.float32),
            pltpu.VMEM((size, size), jnp.float32),
            pltpu.SemaphoreType.DMA((size // panel + 1,)),
        ],
        compiler_params=pltpu.CompilerParams(vmem_limit_bytes=16 * 1024 * 1024),
    )(gram, sketch)


def solution(mesh):
    n, cores = mesh.shape["rows"], mesh.shape["cols"]

    def body(design, signs, kept):
        sketch, gram = sketch_and_gram(design, signs, kept, n, cores)
        return cholesky(gram, sketch, 1.0 / kept.shape[0], design.shape[1])

    return jax.shard_map(
        body,
        mesh=mesh,
        in_specs=(P("rows", "cols"), P("rows"), P()),
        out_specs=(P("rows", "cols"), P(None, "cols")),
        check_vma=False,
    )
```

```python
import functools
import math

import jax
import jax.numpy as jnp
from jax import lax
from jax.experimental import pallas as pl
from jax.experimental.pallas import tpu as pltpu
from jax.sharding import PartitionSpec as P

MESH = pl.DeviceIdType.MESH
LANES = 128
LOADS = 2


def split_two(values):
    high = values.astype(jnp.bfloat16)
    return high, (values - high.astype(jnp.float32)).astype(jnp.bfloat16)


def sketch_kernel(
    low, scale, early, gathers,
    design_hbm, signs_hbm, kept_hbm, sketch_ref, gram_ref,
    design_ref, signs_ref, kept_ref, load_sems, split, buf, one_a, one_b, out_a, out_b, two_a, two_b, gat,
    one_a_send, one_a_recv, one_b_send, one_b_recv, two_a_send, two_a_recv, two_b_send, two_b_recv,
    far_send, far_recv, near_send, near_recv, core_send, core_recv,
):
    me = lax.axis_index("rows")
    core = lax.axis_index("cols")
    high, _, per, width = buf.shape
    loads = [
        pltpu.make_async_copy(kept_hbm, kept_ref, load_sems.at[0]),
        pltpu.make_async_copy(signs_hbm, signs_ref, load_sems.at[1]),
    ]
    chunk = design_ref.shape[0] // LOADS
    for index in range(LOADS):
        piece = pl.ds(index * chunk, chunk)
        loads.append(
            pltpu.make_async_copy(design_hbm.at[piece], design_ref.at[piece], load_sems.at[2 + index])
        )
    for load in loads:
        load.start()
    length = design_ref.shape[0]
    tile = low * per
    spot = me % low
    head, tail = pl.ds(0, early), pl.ds(early, per - early)

    def flip(value, mask):
        bit = 1
        while bit <= mask:
            if mask & bit:
                value = value + (1 - 2 * ((value // bit) % 2)) * bit
            bit *= 2
        return value

    def peer(near, far):
        return flip(me, far * low + near)

    def plane(far):
        return flip(me // low, far)

    def send(src, dst, sems, index, device, other=None):
        return pltpu.make_async_remote_copy(
            src_ref=src, dst_ref=dst, send_sem=sems[0].at[index], recv_sem=sems[1].at[index],
            device_id=(device, core if other is None else other), device_id_type=MESH,
        )

    nears = list(range(low - 1, 0, -1))
    fars = list(range(high - 1, 0, -1))
    closest = sorted(fars, key=lambda far: far > 1)

    barrier = pltpu.get_barrier_semaphore()
    for near in nears:
        pl.semaphore_signal(barrier, inc=1, device_id=(peer(near, 0), core), device_id_type=MESH)
    for far in fars:
        pl.semaphore_signal(barrier, inc=1, device_id=(peer(0, far), core), device_id_type=MESH)
    pl.semaphore_signal(barrier, inc=1, device_id=(me, 1 - core), device_id_type=MESH)

    def one_a_copy(far, near):
        return send(
            buf.at[far, flip(spot, near), head], one_a.at[far, near], (one_a_send, one_a_recv), (far, near),
            peer(near, 0),
        )

    def one_b_copy(far):
        return send(buf.at[far, :, tail], one_b.at[far], (one_b_send, one_b_recv), far, peer(0, far))

    def two_a_copy(far):
        return send(out_a.at[far], two_a.at[far], (two_a_send, two_a_recv), far, peer(0, far))

    def two_b_copy(near):
        return send(
            out_b.at[flip(spot, near)], two_b.at[near], (two_b_send, two_b_recv), near, peer(near, 0)
        )

    def rows_of(part):
        return pl.ds(gathers[part][1], gathers[part][2])

    def near_copy(part, far, near):
        ref = gat.at[core, peer(0, far), rows_of(part)]
        return send(ref, ref, (near_send, near_recv), (part, far, near), peer(near, 0))

    def far_copy(part, far):
        if gathers[part][0]:
            ref = gat.at[core, me, rows_of(part)]
        else:
            ref = gat.at[core, pl.ds((me // low) * low, low), rows_of(part)]
        return send(ref, ref, (far_send, far_recv), (part, far), peer(0, far))

    def core_copy(part, far):
        ref = gat.at[core, pl.ds(plane(far) * low, low), rows_of(part)]
        return send(ref, ref, (core_send, core_recv), (part, far), me, 1 - core)

    def begin(part):
        if gathers[part][0]:
            for far in closest:
                far_copy(part, far).start()
        for near in nears:
            near_copy(part, 0, near).start()

    def middle(part, far):
        if gathers[part][0]:
            far_copy(part, far).wait_recv()
            for near in nears:
                near_copy(part, far, near).start()
        else:
            for near in nears:
                near_copy(part, 0, near).wait_recv()
            for other in closest:
                far_copy(part, other).start()
            core_copy(part, 0).start()

    def finish(part, far):
        if gathers[part][0]:
            for near in nears:
                near_copy(part, far, near).wait_recv()
        else:
            far_copy(part, far).wait_recv()
        core_copy(part, far).start()

    first_row = me * length
    lane = lax.broadcasted_iota(jnp.int32, (LANES, LANES), 1)
    step_rows = min(tile, 256)

    def transform_rows(far, start):
        stacked = []
        for piece in range(step_rows // LANES):
            row = kept_ref[pl.ds(plane(far) * (tile // LANES) + start // LANES + piece, 1), :]
            column = jnp.broadcast_to(row, (LANES, LANES)).T
            blocks = []
            for block in range(length // LANES):
                common = jnp.bitwise_and(column, lane + (first_row + block * LANES))
                odd = jnp.bitwise_and(lax.population_count(common), 1)
                flips = signs_ref[block : block + 1, :]
                entry = (1 - 2 * odd) * flips
                blocks.append(entry.astype(jnp.float32).astype(jnp.bfloat16))
            stacked.append(jnp.concatenate(blocks, axis=1))
        table = jnp.concatenate(stacked, axis=0)
        if far == fars[0] and start == 0:
            for index in range(LOADS):
                loads[2 + index].wait()
                piece = slice(index * chunk, (index + 1) * chunk)
                split[0, piece], split[1, piece] = split_two(design_ref[piece])
        total = jnp.dot(table, split[1], preferred_element_type=jnp.float32)
        total += jnp.dot(table, split[0], preferred_element_type=jnp.float32)
        owner = start // per
        buf[far, owner : owner + step_rows // per] = (total * scale).reshape(step_rows // per, per, width)

    loads[0].wait()
    loads[1].wait()
    for far in fars + [0]:
        for start in range(0, tile, step_rows):
            transform_rows(far, start)
        if far == fars[0]:
            pl.semaphore_wait(barrier, len(nears) + len(fars) + 1)
        for near in nears:
            one_a_copy(far, near).start()
        if far:
            one_b_copy(far).start()

    def near_sum(far):
        total = buf[far, spot, head]
        for near in nears:
            one_a_copy(far, near).wait_recv()
            total += one_a[far, near]
        return total

    for far in fars:
        out_a[far] = near_sum(far)
        two_a_copy(far).start()
    total = buf[0, :, tail]
    for far in fars:
        one_b_copy(far).wait_recv()
        total += one_b[far]
    out_b[...] = total
    for near in nears:
        two_b_copy(near).start()
    total = near_sum(0)
    for far in fars:
        two_a_copy(far).wait_recv()
        total += two_a[far]
    sketch_ref[head, :] = total
    gat[core, me, head] = total
    for part in [part for part in range(len(gathers)) if gathers[part][1] < early]:
        begin(part)
    total = out_b[spot]
    for near in nears:
        two_b_copy(near).wait_recv()
        total += two_b[near]
    sketch_ref[tail, :] = total
    gat[core, me, tail] = total
    for part in [part for part in range(len(gathers)) if gathers[part][1] >= early]:
        begin(part)

    def add_gram(far, first):
        for part in range(len(gathers)):
            core_copy(part, far).wait_recv()
        owners = pl.ds(plane(far) * low, low)
        rows = jnp.concatenate([gat[side, owners].reshape(tile, width) for side in range(gat.shape[0])], axis=1)
        half = rows.shape[1] // 2
        upper, rest = split_two(rows)
        left = jnp.concatenate([upper, upper, rest], axis=0)
        right = jnp.concatenate([upper, rest, upper], axis=0)
        dims = (((0,), (0,)), ((), ()))
        a = lax.dot_general(left[:, :half], right, dims, preferred_element_type=jnp.float32)
        c = lax.dot_general(left[:, half:], right[:, half:], dims, preferred_element_type=jnp.float32)
        gram_ref[0:half, :] = a if first else gram_ref[0:half, :] + a
        gram_ref[half:, half:] = c if first else gram_ref[half:, half:] + c

    passed = [part for part in range(len(gathers)) if gathers[part][0]]
    for index, far in enumerate(closest):
        for part in passed:
            middle(part, far)
            if index == 0:
                finish(part, 0)
                if part == passed[0]:
                    for other in range(len(gathers)):
                        if other not in passed:
                            middle(other, 0)
    ready = 0
    for far in closest:
        for part in range(len(gathers)):
            finish(part, far)
        add_gram(ready, ready == 0)
        ready = far
    add_gram(ready, ready == 0)

    for far in range(high):
        for near in nears:
            one_a_copy(far, near).wait_send()
        if far:
            one_b_copy(far).wait_send()
            two_a_copy(far).wait_send()
        for part in range(len(gathers)):
            core_copy(part, far).wait_send()
            if far:
                far_copy(part, far).wait_send()
            if gathers[part][0] or far == 0:
                for near in nears:
                    near_copy(part, far, near).wait_send()
    for near in nears:
        two_b_copy(near).wait_send()


def sketch_and_gram(design, signs, kept, n, cores):
    length, width = design.shape
    count = kept.shape[0]
    per = count // n
    low = 1 << ((n.bit_length() - 1) // 2)
    high = n // low
    early = per - per // 4
    eighth = per // 8
    gathers = ((0, 0, eighth), (1, eighth, early - eighth), (1, early, per - early))
    whole = width * cores
    sems = []
    count_g = len(gathers)
    for shape in ((high, low), (high,), (high,), (low,), (count_g, high), (count_g, high, low), (count_g, high)):
        sems += [pltpu.SemaphoreType.DMA(shape)] * 2
    late = per - early
    limit = min(60 * 1024 * 1024, 4 * (7 * count * width + 3 * length * width + whole * whole) + 12 * 1024 * 1024)
    return pl.pallas_call(
        functools.partial(sketch_kernel, low, 1.0 / math.sqrt(length * n), early, gathers),
        out_shape=(
            jax.ShapeDtypeStruct((per, width), jnp.float32),
            jax.ShapeDtypeStruct((whole, whole), jnp.float32),
        ),
        in_specs=[pl.BlockSpec(memory_space=pltpu.HBM)] * 3,
        out_specs=(pl.BlockSpec(memory_space=pltpu.VMEM),) * 2,
        scratch_shapes=[
            pltpu.VMEM((length, width), jnp.float32),
            pltpu.VMEM((length // LANES, LANES), jnp.int32),
            pltpu.VMEM((count // LANES, LANES), jnp.int32),
            pltpu.SemaphoreType.DMA((2 + LOADS,)),
            pltpu.VMEM((2, length, width), jnp.bfloat16),
            pltpu.VMEM((high, low, per, width), jnp.float32),
            pltpu.VMEM((high, low, early, width), jnp.float32),
            pltpu.VMEM((high, low, late, width), jnp.float32),
            pltpu.VMEM((high, early, width), jnp.float32),
            pltpu.VMEM((low, late, width), jnp.float32),
            pltpu.VMEM((high, early, width), jnp.float32),
            pltpu.VMEM((low, late, width), jnp.float32),
            pltpu.VMEM((cores, n, per, width), jnp.float32),
            *sems,
        ],
        compiler_params=pltpu.CompilerParams(
            collective_id=0, has_side_effects=True, vmem_limit_bytes=limit
        ),
    )(*(pltpu.with_memory_space_constraint(x, pltpu.HBM) for x in (design, signs.reshape(-1, LANES), kept.reshape(-1, LANES))))


def spread(x, lane):
    return jnp.broadcast_to(x[:, lane:lane+1], x.shape)

def factor_panel(rows, first, reach):
    depth = len(rows)
    size = 8 * depth
    sub = lax.broadcasted_iota(jnp.int32, (8, LANES), 0)
    rows = [list(r) for r in rows]
    columns = {}

    def fetch(j):
        if j < size:
            columns[j] = [spread(rows[r][0], first + j) for r in range(j // 8, depth)]

    for j in range(reach + 1):
        fetch(j)
    for i in range(size):
        g, j = i // 8, i % 8
        column = columns.pop(i)
        root = jnp.broadcast_to(lax.rsqrt(column[0])[j : j + 1], (8, LANES))
        scaled = [c * root for c in column]
        for later in range(i + 1, min(i + reach, size - 1) + 1):
            q = later // 8
            if q == g and later == i + 1:
                weight = columns[later][0][j : j + 1] * root
            else:
                weight = scaled[q - g][later % 8 : later % 8 + 1]
            columns[later] = [c - s * weight for c, s in zip(columns[later], scaled[q - g :])]
        below = jnp.where(sub > j, scaled[0], 0.0)
        lines = [t[j : j + 1] * root for t in rows[g]]
        rows[g] = [jnp.where(sub == j, l, t - below * l) for t, l in zip(rows[g], lines)]
        for r in range(g + 1, depth):
            rows[r] = [x - scaled[r - g] * l for x, l in zip(rows[r], lines)]
        fetch(i + reach + 1)
    return rows


def cholesky_kernel(scale, panel, reach, gram_ref, sketch_ref, sketch_hbm, out_hbm, work, upper, sems):
    size = gram_ref.shape[0]
    width = out_hbm.shape[1]
    tiles = size // LANES
    depth = panel // 8
    lanes = pl.ds(pl.multiple_of(lax.axis_index("cols") * width, width), width)
    copies = [pltpu.make_async_copy(sketch_ref, sketch_hbm, sems.at[size // panel])]
    copies[0].start()
    dims = (((0,), (0,)), ((), ()))
    for start in range(0, size, panel):
        base = start // LANES
        first = start - base * LANES
        source = work if start else gram_ref
        rows = [
            [
                source[start + 8 * r : start + 8 * r + 8, t * LANES : (t + 1) * LANES]
                for t in range(base, tiles)
            ]
            for r in range(depth)
        ]
        done = factor_panel(rows, first, reach)
        full = jnp.concatenate([jnp.concatenate(d, axis=1) for d in done], axis=0)
        row = lax.broadcasted_iota(jnp.int32, full.shape, 0) + first
        column = lax.broadcasted_iota(jnp.int32, full.shape, 1)
        full = jnp.where(row <= column, full, 0.0)
        stop = start + panel
        if base:
            upper[start:stop, : base * LANES] = jnp.zeros((panel, base * LANES), jnp.float32)
        upper[start:stop, base * LANES :] = full * math.sqrt(scale)
        copies.append(
            pltpu.make_async_copy(
                upper.at[start:stop, lanes], out_hbm.at[start:stop], sems.at[start // panel]
            )
        )
        copies[-1].start()
        if stop == size:
            break
        high, low = split_two(full)
        left = jnp.concatenate([high, high, low], axis=0)
        right = jnp.concatenate([high, low, high], axis=0)
        for t in range(stop // LANES, tiles):
            begin = max(stop, t * LANES)
            offset = (t - base) * LANES
            product = lax.dot_general(
                left[:, offset : offset + LANES], right[:, offset:], dims, preferred_element_type=jnp.float32
            )
            place = (slice(begin, (t + 1) * LANES), slice(t * LANES, size))
            work[place] = source[place] - product[begin - t * LANES :]
    for copy in copies:
        copy.wait()


def cholesky(gram, sketch, scale, width, panel=32, reach=12):
    size = gram.shape[0]
    return pl.pallas_call(
        functools.partial(cholesky_kernel, scale, panel, reach),
        out_shape=(
            jax.ShapeDtypeStruct(sketch.shape, jnp.float32),
            jax.ShapeDtypeStruct((size, width), jnp.float32),
        ),
        in_specs=[pl.BlockSpec(memory_space=pltpu.VMEM)] * 2,
        out_specs=(pl.BlockSpec(memory_space=pltpu.HBM),) * 2,
        scratch_shapes=[
            pltpu.VMEM((size, size), jnp.float32),
            pltpu.VMEM((size, size), jnp.float32),
            pltpu.SemaphoreType.DMA((size // panel + 1,)),
        ],
        compiler_params=pltpu.CompilerParams(vmem_limit_bytes=16 * 1024 * 1024),
    )(gram, sketch)


def solution(mesh):
    n, cores = mesh.shape["rows"], mesh.shape["cols"]

    def body(design, signs, kept):
        sketch, gram = sketch_and_gram(design, signs, kept, n, cores)
        return cholesky(gram, sketch, 1.0 / kept.shape[0], design.shape[1])

    return jax.shard_map(
        body,
        mesh=mesh,
        in_specs=(P("rows", "cols"), P("rows"), P()),
        out_specs=(P("rows", "cols"), P(None, "cols")),
        check_vma=False,
    )
```

```python
import functools
import math

import jax
import jax.numpy as jnp
from jax import lax
from jax.experimental import pallas as pl
from jax.experimental.pallas import tpu as pltpu
from jax.sharding import PartitionSpec as P

MESH = pl.DeviceIdType.MESH
LANES = 128
LOADS = 2


def split_two(values):
    high = values.astype(jnp.bfloat16)
    return high, (values - high.astype(jnp.float32)).astype(jnp.bfloat16)


def sketch_kernel(
    low, scale, early, gathers,
    design_hbm, signs_hbm, kept_hbm, sketch_ref, gram_ref,
    design_ref, signs_ref, kept_ref, load_sems, split, buf, one_a, one_b, out_a, out_b, two_a, two_b, gat,
    one_a_send, one_a_recv, one_b_send, one_b_recv, two_a_send, two_a_recv, two_b_send, two_b_recv,
    far_send, far_recv, near_send, near_recv, core_send, core_recv,
):
    me = lax.axis_index("rows")
    core = lax.axis_index("cols")
    high, _, per, width = buf.shape
    loads = [
        pltpu.make_async_copy(kept_hbm, kept_ref, load_sems.at[0]),
        pltpu.make_async_copy(signs_hbm, signs_ref, load_sems.at[1]),
    ]
    chunk = design_ref.shape[0] // LOADS
    for index in range(LOADS):
        piece = pl.ds(index * chunk, chunk)
        loads.append(
            pltpu.make_async_copy(design_hbm.at[piece], design_ref.at[piece], load_sems.at[2 + index])
        )
    for load in loads:
        load.start()
    length = design_ref.shape[0]
    tile = low * per
    spot = me % low
    head, tail = pl.ds(0, early), pl.ds(early, per - early)

    def flip(value, mask):
        bit = 1
        while bit <= mask:
            if mask & bit:
                value = value + (1 - 2 * ((value // bit) % 2)) * bit
            bit *= 2
        return value

    def peer(near, far):
        return flip(me, far * low + near)

    def plane(far):
        return flip(me // low, far)

    def send(src, dst, sems, index, device, other=None):
        return pltpu.make_async_remote_copy(
            src_ref=src, dst_ref=dst, send_sem=sems[0].at[index], recv_sem=sems[1].at[index],
            device_id=(device, core if other is None else other), device_id_type=MESH,
        )

    nears = list(range(low - 1, 0, -1))
    fars = list(range(high - 1, 0, -1))
    closest = sorted(fars, key=lambda far: far > 1)

    barrier = pltpu.get_barrier_semaphore()
    for near in nears:
        pl.semaphore_signal(barrier, inc=1, device_id=(peer(near, 0), core), device_id_type=MESH)
    for far in fars:
        pl.semaphore_signal(barrier, inc=1, device_id=(peer(0, far), core), device_id_type=MESH)
    pl.semaphore_signal(barrier, inc=1, device_id=(me, 1 - core), device_id_type=MESH)

    def one_a_copy(far, near):
        return send(
            buf.at[far, flip(spot, near), head], one_a.at[far, near], (one_a_send, one_a_recv), (far, near),
            peer(near, 0),
        )

    def one_b_copy(far):
        return send(buf.at[far, :, tail], one_b.at[far], (one_b_send, one_b_recv), far, peer(0, far))

    def two_a_copy(far):
        return send(out_a.at[far], two_a.at[far], (two_a_send, two_a_recv), far, peer(0, far))

    def two_b_copy(near):
        return send(
            out_b.at[flip(spot, near)], two_b.at[near], (two_b_send, two_b_recv), near, peer(near, 0)
        )

    def rows_of(part):
        return pl.ds(gathers[part][1], gathers[part][2])

    def near_copy(part, far, near):
        ref = gat.at[core, peer(0, far), rows_of(part)]
        return send(ref, ref, (near_send, near_recv), (part, far, near), peer(near, 0))

    def far_copy(part, far):
        if gathers[part][0]:
            ref = gat.at[core, me, rows_of(part)]
        else:
            ref = gat.at[core, pl.ds((me // low) * low, low), rows_of(part)]
        return send(ref, ref, (far_send, far_recv), (part, far), peer(0, far))

    def core_copy(part, far):
        ref = gat.at[core, pl.ds(plane(far) * low, low), rows_of(part)]
        return send(ref, ref, (core_send, core_recv), (part, far), me, 1 - core)

    def begin(part):
        if gathers[part][0]:
            for far in closest:
                far_copy(part, far).start()
        for near in nears:
            near_copy(part, 0, near).start()

    def middle(part, far):
        if gathers[part][0]:
            far_copy(part, far).wait_recv()
            for near in nears:
                near_copy(part, far, near).start()
        else:
            for near in nears:
                near_copy(part, 0, near).wait_recv()
            for other in closest:
                far_copy(part, other).start()
            core_copy(part, 0).start()

    def finish(part, far):
        if gathers[part][0]:
            for near in nears:
                near_copy(part, far, near).wait_recv()
        else:
            far_copy(part, far).wait_recv()
        core_copy(part, far).start()

    first_row = me * length
    lane = lax.broadcasted_iota(jnp.int32, (LANES, LANES), 1)
    step_rows = min(tile, 256)

    def transform_rows(far, start):
        stacked = []
        for piece in range(step_rows // LANES):
            row = kept_ref[pl.ds(plane(far) * (tile // LANES) + start // LANES + piece, 1), :]
            column = jnp.broadcast_to(row, (LANES, LANES)).T
            blocks = []
            for block in range(length // LANES):
                common = jnp.bitwise_and(column, lane + (first_row + block * LANES))
                odd = jnp.bitwise_and(lax.population_count(common), 1)
                flips = signs_ref[block : block + 1, :]
                entry = (1 - 2 * odd) * flips
                blocks.append(entry.astype(jnp.float32).astype(jnp.bfloat16))
            stacked.append(jnp.concatenate(blocks, axis=1))
        table = jnp.concatenate(stacked, axis=0)
        if far == fars[0] and start == 0:
            for index in range(LOADS):
                loads[2 + index].wait()
                piece = slice(index * chunk, (index + 1) * chunk)
                split[0, piece], split[1, piece] = split_two(design_ref[piece])
        total = jnp.dot(table, split[1], preferred_element_type=jnp.float32)
        total += jnp.dot(table, split[0], preferred_element_type=jnp.float32)
        owner = start // per
        buf[far, owner : owner + step_rows // per] = (total * scale).reshape(step_rows // per, per, width)

    loads[0].wait()
    loads[1].wait()
    for far in fars + [0]:
        for start in range(0, tile, step_rows):
            transform_rows(far, start)
        if far == fars[0]:
            pl.semaphore_wait(barrier, len(nears) + len(fars) + 1)
        for near in nears:
            one_a_copy(far, near).start()
        if far:
            one_b_copy(far).start()

    def near_sum(far):
        total = buf[far, spot, head]
        for near in nears:
            one_a_copy(far, near).wait_recv()
            total += one_a[far, near]
        return total

    for far in fars:
        out_a[far] = near_sum(far)
        two_a_copy(far).start()
    total = buf[0, :, tail]
    for far in fars:
        one_b_copy(far).wait_recv()
        total += one_b[far]
    out_b[...] = total
    for near in nears:
        two_b_copy(near).start()
    total = near_sum(0)
    for far in fars:
        two_a_copy(far).wait_recv()
        total += two_a[far]
    sketch_ref[head, :] = total
    gat[core, me, head] = total
    for part in [part for part in range(len(gathers)) if gathers[part][1] < early]:
        begin(part)
    total = out_b[spot]
    for near in nears:
        two_b_copy(near).wait_recv()
        total += two_b[near]
    sketch_ref[tail, :] = total
    gat[core, me, tail] = total
    for part in [part for part in range(len(gathers)) if gathers[part][1] >= early]:
        begin(part)

    def add_gram(far, first):
        for part in range(len(gathers)):
            core_copy(part, far).wait_recv()
        owners = pl.ds(plane(far) * low, low)
        rows = jnp.concatenate([gat[side, owners].reshape(tile, width) for side in range(gat.shape[0])], axis=1)
        half = rows.shape[1] // 2
        upper, rest = split_two(rows)
        left = jnp.concatenate([upper, upper, rest], axis=0)
        right = jnp.concatenate([upper, rest, upper], axis=0)
        dims = (((0,), (0,)), ((), ()))
        a = lax.dot_general(left[:, :half], right, dims, preferred_element_type=jnp.float32)
        c = lax.dot_general(left[:, half:], right[:, half:], dims, preferred_element_type=jnp.float32)
        gram_ref[0:half, :] = a if first else gram_ref[0:half, :] + a
        gram_ref[half:, half:] = c if first else gram_ref[half:, half:] + c

    passed = [part for part in range(len(gathers)) if gathers[part][0]]
    for index, far in enumerate(closest):
        for part in passed:
            middle(part, far)
            if index == 0:
                finish(part, 0)
                if part == passed[0]:
                    for other in range(len(gathers)):
                        if other not in passed:
                            middle(other, 0)
    ready = 0
    for far in closest:
        for part in sorted(range(len(gathers)), key=lambda part: part not in passed):
            finish(part, far)
        add_gram(ready, ready == 0)
        ready = far
    add_gram(ready, ready == 0)

    for far in range(high):
        for near in nears:
            one_a_copy(far, near).wait_send()
        if far:
            one_b_copy(far).wait_send()
            two_a_copy(far).wait_send()
        for part in range(len(gathers)):
            core_copy(part, far).wait_send()
            if far:
                far_copy(part, far).wait_send()
            if gathers[part][0] or far == 0:
                for near in nears:
                    near_copy(part, far, near).wait_send()
    for near in nears:
        two_b_copy(near).wait_send()


def sketch_and_gram(design, signs, kept, n, cores):
    length, width = design.shape
    count = kept.shape[0]
    per = count // n
    low = 1 << ((n.bit_length() - 1) // 2)
    high = n // low
    early = per - per // 4
    eighth = per // 8
    gathers = ((0, 0, eighth), (1, eighth, early - eighth), (1, early, per - early))
    whole = width * cores
    sems = []
    count_g = len(gathers)
    for shape in ((high, low), (high,), (high,), (low,), (count_g, high), (count_g, high, low), (count_g, high)):
        sems += [pltpu.SemaphoreType.DMA(shape)] * 2
    late = per - early
    limit = min(60 * 1024 * 1024, 4 * (7 * count * width + 3 * length * width + whole * whole) + 12 * 1024 * 1024)
    return pl.pallas_call(
        functools.partial(sketch_kernel, low, 1.0 / math.sqrt(length * n), early, gathers),
        out_shape=(
            jax.ShapeDtypeStruct((per, width), jnp.float32),
            jax.ShapeDtypeStruct((whole, whole), jnp.float32),
        ),
        in_specs=[pl.BlockSpec(memory_space=pltpu.HBM)] * 3,
        out_specs=(pl.BlockSpec(memory_space=pltpu.VMEM),) * 2,
        scratch_shapes=[
            pltpu.VMEM((length, width), jnp.float32),
            pltpu.VMEM((length // LANES, LANES), jnp.int32),
            pltpu.VMEM((count // LANES, LANES), jnp.int32),
            pltpu.SemaphoreType.DMA((2 + LOADS,)),
            pltpu.VMEM((2, length, width), jnp.bfloat16),
            pltpu.VMEM((high, low, per, width), jnp.float32),
            pltpu.VMEM((high, low, early, width), jnp.float32),
            pltpu.VMEM((high, low, late, width), jnp.float32),
            pltpu.VMEM((high, early, width), jnp.float32),
            pltpu.VMEM((low, late, width), jnp.float32),
            pltpu.VMEM((high, early, width), jnp.float32),
            pltpu.VMEM((low, late, width), jnp.float32),
            pltpu.VMEM((cores, n, per, width), jnp.float32),
            *sems,
        ],
        compiler_params=pltpu.CompilerParams(
            collective_id=0, has_side_effects=True, vmem_limit_bytes=limit
        ),
    )(*(pltpu.with_memory_space_constraint(x, pltpu.HBM) for x in (design, signs.reshape(-1, LANES), kept.reshape(-1, LANES))))


def spread(x, lane):
    return jnp.broadcast_to(x[:, lane:lane+1], x.shape)

def factor_panel(rows, first, reach):
    depth = len(rows)
    size = 8 * depth
    sub = lax.broadcasted_iota(jnp.int32, (8, LANES), 0)
    rows = [list(r) for r in rows]
    columns = {}

    def fetch(j):
        if j < size:
            columns[j] = [spread(rows[r][0], first + j) for r in range(j // 8, depth)]

    for j in range(reach + 1):
        fetch(j)
    for i in range(size):
        g, j = i // 8, i % 8
        column = columns.pop(i)
        root = jnp.broadcast_to(lax.rsqrt(column[0])[j : j + 1], (8, LANES))
        scaled = [c * root for c in column]
        for later in range(i + 1, min(i + reach, size - 1) + 1):
            q = later // 8
            if q == g and later == i + 1:
                weight = columns[later][0][j : j + 1] * root
            else:
                weight = scaled[q - g][later % 8 : later % 8 + 1]
            columns[later] = [c - s * weight for c, s in zip(columns[later], scaled[q - g :])]
        below = jnp.where(sub > j, scaled[0], 0.0)
        lines = [t[j : j + 1] * root for t in rows[g]]
        rows[g] = [jnp.where(sub == j, l, t - below * l) for t, l in zip(rows[g], lines)]
        for r in range(g + 1, depth):
            rows[r] = [x - scaled[r - g] * l for x, l in zip(rows[r], lines)]
        fetch(i + reach + 1)
    return rows


def cholesky_kernel(scale, panel, reach, gram_ref, sketch_ref, sketch_hbm, out_hbm, work, upper, sems):
    size = gram_ref.shape[0]
    width = out_hbm.shape[1]
    tiles = size // LANES
    depth = panel // 8
    lanes = pl.ds(pl.multiple_of(lax.axis_index("cols") * width, width), width)
    copies = [pltpu.make_async_copy(sketch_ref, sketch_hbm, sems.at[size // panel])]
    copies[0].start()
    dims = (((0,), (0,)), ((), ()))
    for start in range(0, size, panel):
        base = start // LANES
        first = start - base * LANES
        source = work if start else gram_ref
        rows = [
            [
                source[start + 8 * r : start + 8 * r + 8, t * LANES : (t + 1) * LANES]
                for t in range(base, tiles)
            ]
            for r in range(depth)
        ]
        done = factor_panel(rows, first, reach)
        full = jnp.concatenate([jnp.concatenate(d, axis=1) for d in done], axis=0)
        row = lax.broadcasted_iota(jnp.int32, full.shape, 0) + first
        column = lax.broadcasted_iota(jnp.int32, full.shape, 1)
        full = jnp.where(row <= column, full, 0.0)
        stop = start + panel
        if base:
            upper[start:stop, : base * LANES] = jnp.zeros((panel, base * LANES), jnp.float32)
        upper[start:stop, base * LANES :] = full * math.sqrt(scale)
        copies.append(
            pltpu.make_async_copy(
                upper.at[start:stop, lanes], out_hbm.at[start:stop], sems.at[start // panel]
            )
        )
        copies[-1].start()
        if stop == size:
            break
        high, low = split_two(full)
        left = jnp.concatenate([high, high, low], axis=0)
        right = jnp.concatenate([high, low, high], axis=0)
        for t in range(stop // LANES, tiles):
            begin = max(stop, t * LANES)
            offset = (t - base) * LANES
            product = lax.dot_general(
                left[:, offset : offset + LANES], right[:, offset:], dims, preferred_element_type=jnp.float32
            )
            place = (slice(begin, (t + 1) * LANES), slice(t * LANES, size))
            work[place] = source[place] - product[begin - t * LANES :]
    for copy in copies:
        copy.wait()


def cholesky(gram, sketch, scale, width, panel=32, reach=12):
    size = gram.shape[0]
    return pl.pallas_call(
        functools.partial(cholesky_kernel, scale, panel, reach),
        out_shape=(
            jax.ShapeDtypeStruct(sketch.shape, jnp.float32),
            jax.ShapeDtypeStruct((size, width), jnp.float32),
        ),
        in_specs=[pl.BlockSpec(memory_space=pltpu.VMEM)] * 2,
        out_specs=(pl.BlockSpec(memory_space=pltpu.HBM),) * 2,
        scratch_shapes=[
            pltpu.VMEM((size, size), jnp.float32),
            pltpu.VMEM((size, size), jnp.float32),
            pltpu.SemaphoreType.DMA((size // panel + 1,)),
        ],
        compiler_params=pltpu.CompilerParams(vmem_limit_bytes=16 * 1024 * 1024),
    )(gram, sketch)


def solution(mesh):
    n, cores = mesh.shape["rows"], mesh.shape["cols"]

    def body(design, signs, kept):
        sketch, gram = sketch_and_gram(design, signs, kept, n, cores)
        return cholesky(gram, sketch, 1.0 / kept.shape[0], design.shape[1])

    return jax.shard_map(
        body,
        mesh=mesh,
        in_specs=(P("rows", "cols"), P("rows"), P()),
        out_specs=(P("rows", "cols"), P(None, "cols")),
        check_vma=False,
    )
```
